32 devices in a mesh: seq: 8 (over y, x, core), mp: 4 (over z).
Axes of the slice: x: 2, y: 2, z: 4, core: 2. Of those that a mesh axis runs over, the one named last changes fastest.
Arguments:
- inputs: bfloat16 [8192, 4096], P('seq', 'mp'), may hold values from -6 to 6
- conv_weight: bfloat16 [4, 4096], P(None, 'mp'), may hold values from -3 to 3
- conv_bias: bfloat16 [4096], P('mp'), may hold values from -3 to 3
- doc_start: int32 [8192], P('seq'), may hold values from 0 to 8191, as said below
- counts: int32 [8], P('seq'), may hold values from 341 to 1024
Outputs:
- gram: float32 [4096, 4096], P('seq', 'mp')
The draws below stay inside these ranges and needn't reach their ends.
Inputs may be any that keep to these rules, and one draw needn't show every extreme that they name: doc_start is never above the token's own position, and for t > 0 either doc_start[t] == t or doc_start[t] == doc_start[t - 1]; doc_start[0] is 0.
All inputs are finite; a program needn't handle non-finite values.
Results may differ from the reference program's by a relative error of at most 0.0003.
Values may be sent and summed in bfloat16 or wider, within the bound.
A program may use at most 64 MiB of HBM per device.

```python
import jax
import jax.numpy as jnp
from jax import lax

C = 4096
KERNEL = 4
TOK_DEV = 1024
TOKENS = 8192
SHARDS = 8


def draw_doc_start(key, part):
    flags = jax.random.randint(key, (TOKENS,), 0, max(TOK_DEV // 4, 2)) == 0
    flags = flags.at[0].set(True).at[TOKENS - 1].set(True)
    position = jnp.arange(TOKENS, dtype=jnp.int32)
    starts = jnp.where(flags, position, 0)
    return lax.cummax(starts, axis=0).astype(jnp.int32)


def draw_counts(key, part):
    shard_ids = jnp.arange(SHARDS, dtype=jnp.int32)
    spread = TOK_DEV - TOK_DEV // 3 - TOK_DEV // 8
    base = TOK_DEV // 3 + shard_ids * spread // (SHARDS - 1)
    jitter = jax.random.randint(key, (SHARDS,), 0, TOK_DEV // 8 + 1)
    values = jnp.minimum(base + jitter, TOK_DEV)
    return values.at[SHARDS - 1].set(TOK_DEV).astype(jnp.int32)


def block_scale(key, dims, pieces, low, top_value):
    loudness, own = 1.0, jax.random.fold_in(key, 6)
    for axis_at, blocks in pieces:
        draws = jnp.exp(jax.random.uniform(jax.random.fold_in(own, axis_at), (blocks,), jnp.float32, low / len(pieces), top_value / len(pieces)))
        loudness = loudness * jnp.repeat(draws, dims[axis_at] // blocks).reshape([-1 if axis == axis_at else 1 for axis in range(len(dims))])
    return loudness


def gaussian(stream_key, extent, scale, most, split=(), kind=jnp.bfloat16):
    entries = jax.random.normal(stream_key, extent, jnp.float32) * scale
    if len(split) > 0:
        entries = block_scale(stream_key, extent, split, -0.22, 0.18) * entries
    return jnp.clip(entries, min=-most, max=most).astype(kind)


def setup_inputs(seed: int = 0) -> dict:
    seeds = jax.random.split(jax.random.key(seed), 6)
    return {
        "inputs": gaussian(seeds[0], (TOKENS, C), 1.0, 6.0, ((0, 8), (1, 4))),
        "conv_weight": gaussian(seeds[1], (KERNEL, C), KERNEL ** -0.5, 3.0, ((1, 4),)),
        "conv_bias": gaussian(seeds[2], (C,), 0.5, 3.0, ((0, 4),)),
        "doc_start": draw_doc_start(jax.random.fold_in(seeds[5], 71), 0),
        "counts": draw_counts(jax.random.fold_in(seeds[5], 71), 0),
    }


def causal_conv(extended, weights, bias, position, doc_start, length):
    kernel_len = weights.shape[0]
    summed = jnp.zeros((length, weights.shape[1]), jnp.float32) + bias.astype(jnp.float32)
    for lag in range(kernel_len):
        window = extended[kernel_len - 1 - lag: kernel_len - 1 - lag + length].astype(jnp.float32)
        usable = (position - lag) >= doc_start
        summed = summed + jnp.where(usable[:, None], weights[lag].astype(jnp.float32) * window, 0.0)
    return jax.nn.silu(summed).astype(jnp.bfloat16)


def reference(inputs, conv_weight, conv_bias, doc_start, counts):
    position = jnp.arange(TOKENS, dtype=jnp.int32)
    padding = jnp.zeros((KERNEL - 1, C), jnp.bfloat16)
    extended = jnp.concatenate([padding, inputs], axis=0)
    feats = causal_conv(extended, conv_weight, conv_bias, position, doc_start, TOKENS)
    counted = (position % TOK_DEV) < jnp.repeat(counts, TOK_DEV)
    kept = jnp.where(counted[:, None], feats, jnp.zeros_like(feats))

    def add_block(carry, pair):
        left, right = pair
        return carry + lax.dot_general(left, right, (((0,), (0,)), ((), ())), preferred_element_type=jnp.float32), None

    summed, _ = lax.scan(add_block, jnp.zeros((C, C), jnp.float32),
                         (feats.reshape(SHARDS, TOK_DEV, C), kept.reshape(SHARDS, TOK_DEV, C)))
    token_total = jnp.sum(counts.astype(jnp.float32))
    return summed / token_total
```

```python
import functools

import jax
import jax.numpy as jnp
from jax import lax
from jax.experimental import pallas as pl
from jax.experimental.pallas import tpu as pltpu
from jax.sharding import PartitionSpec as P

MESH = pl.DeviceIdType.MESH
LANES = 128
HALO = 16


def when(cond):
    return pl.when(cond)


def gram_kernel(peers, depth, taps, x_hbm, taps_ref, code_ref, cnt_ref, o_ref, ext, feats, got, part,
                from_x, from_y, sum_y, sum_x, totals,
                load_sem, halo_sem, cnt_send, cnt_recv, pair_send, pair_recv,
                up_send, down_send, fwd_send, got_recv,
                a1_send, a1_recv, b1_send, b1_recv, a2_send, a2_recv, b2_send, b2_recv):
    s, z = lax.axis_index("seq"), lax.axis_index("mp")
    core, x, y = lax.rem(s, 2), lax.rem(s // 2, 2), s // 4
    sib, over_x, over_y = s + 1 - 2 * core, s + 2 - 4 * x, s + 4 - 8 * y
    quad = s // 2
    rows, width = x_hbm.shape
    half = width // 2
    pieces = half // LANES

    def remote(src, dst, send, recv, to):
        return pltpu.make_async_remote_copy(src_ref=src, dst_ref=dst, send_sem=send, recv_sem=recv,
                                            device_id=to, device_id_type=MESH)

    load = pltpu.make_async_copy(x_hbm, ext.at[pl.ds(HALO, rows)], load_sem)
    load.start()

    barrier = pltpu.get_barrier_semaphore()
    for step in range(1, peers):
        pl.semaphore_signal(barrier, inc=1, device_id=(lax.rem(s + step, peers), z), device_id_type=MESH)

    @when(z > 0)
    def _():
        pl.semaphore_signal(barrier, inc=1, device_id=(s, z - 1), device_id_type=MESH)

    @when(z < depth - 1)
    def _():
        pl.semaphore_signal(barrier, inc=1, device_id=(s, z + 1), device_id_type=MESH)

    pl.semaphore_wait(barrier, peers - 1 + jnp.where(z > 0, 1, 0) + jnp.where(z < depth - 1, 1, 0))

    halo = remote(x_hbm.at[pl.ds(rows - HALO, HALO)], ext.at[pl.ds(0, HALO)], halo_sem.at[0], halo_sem.at[1],
                  (lax.rem(s + 1, peers), z))

    @when(s < peers - 1)
    def _():
        halo.start()

    def cnt_copy(step, slot):
        return remote(cnt_ref, totals.at[slot], cnt_send.at[step], cnt_recv.at[slot],
                      (lax.rem(s + step, peers), z))

    for step in range(1, peers):
        cnt_copy(step, s).start()

    load.wait()

    @when(s == 0)
    def _():
        ext[0:HALO, :] = jnp.zeros((HALO, width), ext.dtype)

    @when(s > 0)
    def _():
        halo.wait_recv()

    block = LANES
    own_rows = pl.multiple_of(core * rows, rows)

    def conv(column):
        at = pl.ds(pl.multiple_of(column, LANES), LANES)
        taps_here = taps_ref[:, at]

        def body(r, _):
            first = pl.multiple_of(r * block, block)
            seen = ext[pl.ds(first, block + HALO), at].astype(jnp.float32)
            code = code_ref[pl.ds(first, block), :]
            lags = jnp.bitwise_and(code, taps - 1)
            total = jnp.broadcast_to(taps_here[taps : taps + 1], (block, LANES))
            for lag in range(taps):
                window = (pltpu.roll(seen, lag, 0) if lag else seen)[HALO:]
                term = jnp.broadcast_to(taps_here[lag : lag + 1], (block, LANES)) * window
                total = total + jnp.where(lags >= lag, term, 0.0)
            value = total / (1.0 + jnp.exp(-total))
            value = jnp.where(code >= taps, value, 0.0)
            feats[pl.ds(pl.multiple_of(own_rows + first, block), block), at] = value.astype(feats.dtype)
            return 0

        lax.fori_loop(0, rows // block, body, 0)

    def pair_copy(piece, row0):
        spot = feats.at[pl.ds(row0, rows), pl.ds(pl.multiple_of(piece * LANES, LANES), LANES)]
        return remote(spot, spot, pair_send.at[piece], pair_recv.at[piece], (sib, z))

    def own_piece(k):
        return feats.at[:, pl.ds(pl.multiple_of(core * half + k * LANES, LANES), LANES)]

    def up_copy(k):
        return remote(own_piece(k), got.at[z, k], up_send.at[k], got_recv.at[z, k], (s, lax.rem(z + 1, depth)))

    def down_copy(k):
        return remote(own_piece(k), got.at[z, k], down_send.at[k], got_recv.at[z, k],
                      (s, lax.rem(z + depth - 1, depth)))

    def spread(k, _):
        for side in (1 - core, core):
            piece = side * pieces + k
            conv(piece * LANES)
            pair_copy(piece, own_rows).start()
        pair_copy(core * pieces + k, own_rows).wait_recv()

        @when(z < depth - 1)
        def _():
            up_copy(k).start()

        @when(z > 0)
        def _():
            down_copy(k).start()

        return 0

    lax.fori_loop(0, pieces, spread, 0)

    def settle(k, _):
        pair_copy((1 - core) * pieces + k, own_rows).wait_recv()
        got[z, k] = feats[:, pl.ds(pl.multiple_of(core * half + k * LANES, LANES), LANES)]
        return 0

    lax.fori_loop(0, pieces, settle, 0)

    steps = pieces + 2 * pieces * (depth - 1)

    def place(i):
        later = i - pieces
        own = i < pieces
        later = jnp.where(own, 0, later)
        away = jnp.where(own, 0, later // (2 * pieces) + 1)
        k = jnp.where(own, i, lax.rem(later, 2 * pieces) // 2)
        sign = 1 - 2 * lax.rem(later, 2)
        block_at = z + sign * away
        valid = jnp.logical_and(block_at >= 0, block_at < depth)
        block_in = jnp.where(valid, block_at, 0)
        return away, k, sign, block_in, valid

    def apart(block_at):
        return lax.rem(block_at, 2) != x, block_at // 2 != y

    def fwd_copy(block_at, k, sign):
        to = lax.rem(z - sign + depth, depth)
        return remote(got.at[block_at, k], got.at[block_at, k], fwd_send.at[block_at, k], got_recv.at[block_at, k],
                      (s, to))

    def a1_copy(b, k):
        return remote(part.at[b, k, 0], from_x.at[b, k], a1_send.at[b, k], a1_recv.at[b, k], (over_x, z))

    def b1_copy(b, k):
        return remote(part.at[b, k, 1], from_y.at[b, k], b1_send.at[b, k], b1_recv.at[b, k], (over_y, z))

    def a2_copy(b, k):
        return remote(part.at[b, k, 0], sum_y.at[k], a2_send.at[b, k], a2_recv.at[k], (over_y, z))

    def b2_copy(b, k):
        return remote(part.at[b, k, 1], sum_x.at[k], b2_send.at[b, k], b2_recv.at[k], (over_x, z))

    def product(i):
        away, k, sign, b, valid = place(i)
        beyond = z - sign
        far_x, far_y = apart(b)

        @when(valid)
        def _():
            @when(away > 0)
            def _():
                fwd_copy(b, k, sign).wait_recv()

                @when(jnp.logical_and(beyond >= 0, beyond < depth))
                def _():
                    fwd_copy(b, k, sign).start()

            for side in range(2):
                part[b, k, side] = lax.dot_general(got[b, k], feats[:, side * half : (side + 1) * half],
                                                   (((0,), (0,)), ((), ())), preferred_element_type=jnp.float32)

            @when(far_x)
            def _():
                a1_copy(b, k).start()

            @when(far_y)
            def _():
                b1_copy(b, k).start()

    def combine(i):
        _, k, _, b, valid = place(i)
        far_x, far_y = apart(b)

        @when(jnp.logical_and(valid, jnp.logical_and(jnp.logical_not(far_x), far_y)))
        def _():
            a1_copy(b, k).wait_recv()
            part[b, k, 0] = part[b, k, 0] + from_x[b, k]
            a2_copy(b, k).start()

        @when(jnp.logical_and(valid, jnp.logical_and(far_x, jnp.logical_not(far_y))))
        def _():
            b1_copy(b, k).wait_recv()
            part[b, k, 1] = part[b, k, 1] + from_y[b, k]
            b2_copy(b, k).start()

    lag = 2

    def main(i, _):
        @when(i < steps)
        def _():
            product(i)

        @when(i >= lag)
        def _():
            combine(i - lag)

        return 0

    lax.fori_loop(0, steps + lag, main, 0)

    for step in range(1, peers):
        cnt_copy(step, lax.rem(s + peers - step, peers)).wait_recv()
    totals[s] = cnt_ref[...]
    token_total = jnp.sum(totals[...].astype(jnp.float32), axis=0)[0:1, :]
    scale = jnp.broadcast_to(jnp.concatenate([1.0 / token_total] * (half // LANES), axis=1), (LANES, half))

    def finish(k, _):
        at = pl.ds(pl.multiple_of(k * LANES, LANES), LANES)
        a1_copy(quad, k).wait_recv()
        a2_copy(quad, k).wait_recv()
        o_ref[at, 0:half] = (part[quad, k, 0] + from_x[quad, k] + sum_y[k]) * scale
        b1_copy(quad, k).wait_recv()
        b2_copy(quad, k).wait_recv()
        o_ref[at, half : 2 * half] = (part[quad, k, 1] + from_y[quad, k] + sum_x[k]) * scale
        return 0

    lax.fori_loop(0, pieces, finish, 0)

    @when(s < peers - 1)
    def _():
        halo.wait_send()

    for step in range(1, peers):
        cnt_copy(step, s).wait_send()

    def sent(k, _):
        for side in range(2):
            pair_copy(side * pieces + k, own_rows).wait_send()

        @when(z < depth - 1)
        def _():
            up_copy(k).wait_send()

        @when(z > 0)
        def _():
            down_copy(k).wait_send()

        return 0

    lax.fori_loop(0, pieces, sent, 0)

    def sent_late(i, _):
        away, k, sign, b, valid = place(i)
        beyond = z - sign
        far_x, far_y = apart(b)

        @when(jnp.logical_and(jnp.logical_and(valid, away > 0), jnp.logical_and(beyond >= 0, beyond < depth)))
        def _():
            fwd_copy(b, k, sign).wait_send()

        @when(jnp.logical_and(valid, far_x))
        def _():
            a1_copy(b, k).wait_send()

        @when(jnp.logical_and(valid, far_y))
        def _():
            b1_copy(b, k).wait_send()

        @when(jnp.logical_and(valid, jnp.logical_and(jnp.logical_not(far_x), far_y)))
        def _():
            a2_copy(b, k).wait_send()

        @when(jnp.logical_and(valid, jnp.logical_and(far_x, jnp.logical_not(far_y))))
        def _():
            b2_copy(b, k).wait_send()

        return 0

    lax.fori_loop(0, steps, sent_late, 0)


def fused_on_device(peers, depth, inputs, conv_weight, conv_bias, doc_start, counts):
    rows, width = inputs.shape
    taps = conv_weight.shape[0]
    half = width // 2
    pieces = half // LANES
    index = jnp.arange(rows, dtype=jnp.int32)
    reach = jnp.minimum(lax.axis_index("seq") * rows + index - doc_start, taps - 1)
    code = reach + jnp.where(index < counts[0], taps, 0)
    code = jnp.broadcast_to(code[:, None], (rows, LANES))
    cnt = jnp.broadcast_to(counts[0], (8, LANES))
    taps_bias = jnp.concatenate([conv_weight, conv_bias[None]], axis=0).astype(jnp.float32)
    vmem = pl.BlockSpec(memory_space=pltpu.VMEM)
    dma = lambda *shape: pltpu.SemaphoreType.DMA(shape)
    f32 = jnp.float32
    grid = (depth, pieces)
    return pl.pallas_call(
        functools.partial(gram_kernel, peers, depth, taps),
        out_shape=jax.ShapeDtypeStruct((half, width), f32),
        in_specs=[pl.BlockSpec(memory_space=pl.ANY), vmem, vmem, vmem],
        out_specs=vmem,
        scratch_shapes=[
            pltpu.VMEM((rows + HALO, width), inputs.dtype),
            pltpu.VMEM((2 * rows, width), inputs.dtype),
            pltpu.VMEM((depth, pieces, 2 * rows, LANES), inputs.dtype),
            pltpu.VMEM((depth, pieces, 2, LANES, half), f32),
            pltpu.VMEM((depth, pieces, LANES, half), f32),
            pltpu.VMEM((depth, pieces, LANES, half), f32),
            pltpu.VMEM((pieces, LANES, half), f32),
            pltpu.VMEM((pieces, LANES, half), f32),
            pltpu.VMEM((peers, 8, LANES), jnp.int32),
            pltpu.SemaphoreType.DMA, dma(2), dma(peers), dma(peers), dma(2 * pieces), dma(2 * pieces),
            dma(pieces), dma(pieces), dma(*grid), dma(*grid),
            dma(*grid), dma(*grid), dma(*grid), dma(*grid), dma(*grid), dma(pieces), dma(*grid), dma(pieces),
        ],
        compiler_params=pltpu.CompilerParams(collective_id=0, has_side_effects=True,
                                             vmem_limit_bytes=60 * 1024 * 1024),
        name="gram",
    )(inputs, taps_bias, code, cnt)


def passed_along(x, axis, by):
    peers = lax.axis_size(axis)
    pairs = [(i, i + by) for i in range(peers) if 0 <= i + by < peers]
    return lax.ppermute(x, axis, pairs)


def causal_conv(extended, weights, bias, position, doc_start, length):
    kernel_len = weights.shape[0]
    summed = jnp.zeros((length, weights.shape[1]), jnp.float32) + bias.astype(jnp.float32)
    for lag in range(kernel_len):
        window = extended[kernel_len - 1 - lag : kernel_len - 1 - lag + length].astype(jnp.float32)
        usable = position - lag >= doc_start
        summed = summed + jnp.where(usable[:, None], weights[lag].astype(jnp.float32) * window, 0.0)
    return jax.nn.silu(summed).astype(jnp.bfloat16)


def on_device(inputs, conv_weight, conv_bias, doc_start, counts):
    row_count = inputs.shape[0]
    kernel_len = conv_weight.shape[0]
    position = lax.axis_index("seq") * row_count + jnp.arange(row_count, dtype=jnp.int32)
    counted = jnp.arange(row_count, dtype=jnp.int32) < counts[0]
    token_total = lax.psum(counts.astype(jnp.float32)[0], "seq")
    prior = passed_along(inputs[row_count - (kernel_len - 1) :], "seq", 1)
    extended = jnp.concatenate([prior, inputs], axis=0)
    own_feats = causal_conv(extended, conv_weight, conv_bias, position, doc_start, row_count)
    kept = jnp.where(counted[:, None], own_feats, jnp.zeros_like(own_feats))
    whole = lax.all_gather(own_feats, "mp", axis=1, tiled=True)
    summed = lax.psum_scatter(
        lax.dot_general(whole, kept, (((0,), (0,)), ((), ())), preferred_element_type=jnp.float32),
        "seq",
        scatter_dimension=0,
        tiled=True,
    )
    return summed / token_total


def solution(mesh):
    placed = (P("seq", "mp"), P(None, "mp"), P("mp"), P("seq"), P("seq"))
    peers, depth = mesh.shape["seq"], mesh.shape["mp"]
    fits = peers == 2 * depth and peers == 2**3
    body = functools.partial(fused_on_device, peers, depth) if fits else on_device
    return jax.shard_map(body, mesh=mesh, in_specs=placed, out_specs=P("seq", "mp"), check_vma=False)
```
